32 devices in a mesh: groups: 2 (over y), range: 8 (over z, x), sub: 2 (over core).
Axes of the slice: x: 2, y: 2, z: 4, core: 2. Of those that a mesh axis runs over, the one named last changes fastest.
Arguments:
- samples: float32 [2, 1024, 32, 128], P(None, ('groups', 'range', 'sub')), parts along dimension 1, may hold values from -6 to 6
- beam_weights: float32 [32, 8, 2, 64, 128], P(('groups', 'range'), None, None, None, 'sub'), parts along dimension 0, may hold values from -0.25 to 0.25
- subarrays: int32 [32, 8, 64], P(('groups', 'range', 'sub')), parts along dimension 0, may hold values from 0 to 511, as said below
- training: int32 [64], P(('groups', 'range', 'sub')), parts along dimension 0, may hold values 0 or 1
Outputs:
- covariance: float32 [32, 8, 64, 128], P(('groups', 'range', 'sub')), parts along dimension 0
- filtered: float32 [2, 128, 64, 128], P(None, None, ('groups', 'range', 'sub')), parts along dimension 2
- energy: float32 [256], P('groups'), parts along dimension 0
The draws below stay inside these ranges and needn't reach their ends.
There are 2 independent parts, one for each index of `groups`. The reference program is written for one: setup_inputs(seed, part) draws one part's arguments, and reference() takes and returns one part's arrays. A program takes and returns all parts, laid end to end along the dimension named above; each array names one. Nothing has to cross between parts.
Inputs may be any that keep to these rules, and one draw needn't show every extreme that they name: `subarrays`: in each gate block the 512 indices are all 512 channels, each once.
All inputs are finite; a program needn't handle non-finite values. No bound on the sum of `training` on one device may be relied on, other than what follows from the above.
Results may differ from the reference program's by a relative error of at most 0.0003.
Values sent between devices are 32-bit elements; how exact they have to be, the bound alone decides.
A program may use at most 64 MiB of HBM per device.

```python
import jax
import jax.numpy as jnp
from jax import lax

C = 512
S = 64
K = 128
P_SIZE = 128
GB = 2
NS = 8
G = 32
NB = 16


def draw_subarrays(key, part):
    several = jax.random.split(jax.random.fold_in(key, 17), NB)
    orders = jax.vmap(lambda single: jax.random.permutation(single, C))(several)
    return orders.reshape(NB, NS, S).astype(jnp.int32)


def plant(values, stream_key, smallest, top_value):
    longest = values.shape.index(max(values.shape))
    spots = []
    for shift in (0, 1):
        where = [jax.random.randint(jax.random.fold_in(stream_key, axis), (), 0, length) for axis, length in enumerate(values.shape)]
        where[longest] = (where[longest] + shift) % values.shape[longest]
        spots.append(tuple(where))
    return values.at[spots[0]].set(smallest).at[spots[1]].set(top_value)


def level_of(rng, extent, cuts, least, high):
    level, own = 1.0, jax.random.fold_in(rng, 6)
    for dim, parts in cuts:
        heights = jnp.exp(jax.random.uniform(jax.random.fold_in(own, dim), (parts,), jnp.float32, least / len(cuts), high / len(cuts)))
        level = level * jnp.repeat(heights, extent[dim] // parts).reshape([-1 if axis == dim else 1 for axis in range(len(extent))])
    return level


def normal_values(key, extent, width, bound, cuts=(), kind=jnp.bfloat16):
    drawn = width * jax.random.normal(key, extent, jnp.float32)
    if cuts:
        drawn = drawn * level_of(key, extent, cuts, -0.22, 0.18)
    return jnp.clip(drawn, -bound, bound).astype(kind)


def setup_inputs(seed: int = 0, part: int = 0) -> dict:
    splits = jax.random.split(jax.random.key(seed), 5)
    part_keys = jax.random.split(jax.random.fold_in(splits[4], part), 5)
    samples = normal_values(part_keys[0], (2, C, G, P_SIZE), 1.0, 6.0, ((1, 16),), jnp.float32)
    beam_weights = normal_values(part_keys[1], (NB, NS, 2, S, K), C ** -0.5, 0.25, ((0, 8), (4, 2)), jnp.float32)
    subarrays = draw_subarrays(jax.random.fold_in(jax.random.fold_in(splits[4], part), 71), part)
    training = plant((jax.random.randint(part_keys[3], (G,), 0, 2) < 1).astype(jnp.int32), jax.random.fold_in(part_keys[3], 1), 0, 1)
    return dict(samples=samples, beam_weights=beam_weights, subarrays=subarrays, training=training)


loading = 0.05

def block_terms(snaps, chosen, weights, masked, factor):
    highest = lax.Precision.HIGHEST
    picked = jnp.take(snaps, chosen, axis=1)
    real_part = picked[0]
    imag_part = picked[1]
    real_masked = real_part * masked
    imag_masked = imag_part * masked
    cov_real = (jnp.einsum('snx,smx->snm', real_masked, real_part, precision=highest) + jnp.einsum('snx,smx->snm', imag_masked, imag_part, precision=highest)) * factor
    cov_imag = (jnp.einsum('snx,smx->snm', imag_masked, real_part, precision=highest) - jnp.einsum('snx,smx->snm', real_masked, imag_part, precision=highest)) * factor
    w_real = weights[:, 0]
    w_imag = weights[:, 1]
    out_real = jnp.einsum('snk,snx->kx', w_real, real_part, precision=highest) + jnp.einsum('snk,snx->kx', w_imag, imag_part, precision=highest)
    out_imag = jnp.einsum('snk,snx->kx', w_real, imag_part, precision=highest) - jnp.einsum('snk,snx->kx', w_imag, real_part, precision=highest)
    prod_real = jnp.einsum('snm,smk->snk', cov_real, w_real, precision=highest) - jnp.einsum('snm,smk->snk', cov_imag, w_imag, precision=highest)
    prod_imag = jnp.einsum('snm,smk->snk', cov_real, w_imag, precision=highest) + jnp.einsum('snm,smk->snk', cov_imag, w_real, precision=highest)
    quadratic = lax.optimization_barrier(jnp.sum(w_real * prod_real + w_imag * prod_imag, axis=(0, 1)))
    inverse = 1.0 / jnp.sqrt(quadratic + loading)
    filtered = jnp.stack([out_real * inverse[:, None], out_imag * inverse[:, None]])
    energy = lax.optimization_barrier(jnp.sum(out_real * out_real + out_imag * out_imag, axis=1))
    covariance = jnp.concatenate([cov_real, cov_imag], axis=-1)
    return (covariance, filtered, energy)

def reference(samples, beam_weights, subarrays, training):
    factor = 1.0 / (GB * P_SIZE)

    def one_block(index):
        start = (index * GB).astype(jnp.int32)
        snaps = lax.dynamic_slice_in_dim(samples, start, GB, 2).reshape(2, C, GB * P_SIZE)
        gates_on = lax.dynamic_slice_in_dim(training, start, GB, 0).astype(jnp.float32)
        masked = jnp.repeat(gates_on, P_SIZE)
        return block_terms(snaps, subarrays[index], beam_weights[index], masked, factor)
    covs, filts, energies = lax.map(one_block, jnp.arange(NB, dtype=jnp.int32))
    filtered = filts.reshape(NB, 2, K, GB, P_SIZE).transpose(1, 2, 0, 3, 4).reshape(2, K, G, P_SIZE)
    energy = lax.optimization_barrier(jnp.sum(energies, axis=0)) / (G * P_SIZE)
    return (covs, filtered, energy)
```

```python
import functools

import jax
import jax.numpy as jnp
from jax import lax
from jax.experimental import pallas as pl
from jax.experimental.pallas import tpu as pltpu
from jax.sharding import PartitionSpec as P

GB = 2
loading = 0.05
F32 = jnp.float32
BF16 = jnp.bfloat16


def split(x):
    hi = x.astype(BF16)
    return hi, (x - hi.astype(F32)).astype(BF16)


def dot(a, b):
    return jnp.dot(a, b, preferred_element_type=F32)


def dot_t(a, b):
    return lax.dot_general(a, b, (((1,), (1,)), ((), ())), preferred_element_type=F32)


def partner(me, step, count):
    other, bit = me, 1
    while bit < count:
        other = other + ((step // bit) % 2) * (1 - 2 * ((me // bit) % 2)) * bit
        bit *= 2
    return other


def kernel(
    dims,
    smp, bw, sub, trn,
    cov, filt, en,
    stage, sendb, recv, wfull, lhs, wst, wq, sacc, gacc, esend, erecv,
    send_sem, recv_sem, wsem, esend_sem, erecv_sem, lsem,
):
    n, cores, c_loc, gates, pulses, ns, s_n, k_half = dims
    beams = 2 * k_half
    chans = n * c_loc
    half = n // 2
    rows = half * c_loc
    core = lax.axis_index("sub")
    me = lax.axis_index("range") * cores + core

    def where(d):
        return {"range": d // cores, "sub": d % cores}

    load = pltpu.make_async_copy(smp, stage, lsem.at[0])
    load.start()
    keep = pltpu.make_async_copy(bw.at[core], wfull.at[core], lsem.at[1])
    keep.start()

    barrier = pltpu.get_barrier_semaphore()

    def greet(t, c):
        pl.semaphore_signal(
            barrier, inc=1, device_id=where(partner(me, t, n)), device_id_type=pl.DeviceIdType.MESH
        )
        return c

    lax.fori_loop(1, n, greet, 0)
    load.wait()

    def arrange(d, c):
        for g in range(GB):
            sendb[d, g * 2 * c_loc : (g + 1) * 2 * c_loc, :] = stage[
                pl.ds(d * GB + g, 2 * c_loc, stride=gates), :
            ]
        return c

    lax.fori_loop(0, n, arrange, 0)
    recv[me] = sendb[me]
    pl.semaphore_wait(barrier, n - 1)

    def piece(d, slot, dev):
        return pltpu.make_async_remote_copy(
            src_ref=sendb.at[d],
            dst_ref=recv.at[slot],
            send_sem=send_sem.at[d],
            recv_sem=recv_sem.at[slot],
            device_id=where(dev),
            device_id_type=pl.DeviceIdType.MESH,
        )

    def launch(t, c):
        d = partner(me, t, n)
        piece(d, me, d).start()
        return c

    lax.fori_loop(1, n, launch, 0)
    swap = pltpu.make_async_remote_copy(
        src_ref=bw.at[1 - core],
        dst_ref=wfull.at[core],
        send_sem=wsem.at[0],
        recv_sem=wsem.at[1],
        device_id={"sub": 1 - core},
        device_id_type=pl.DeviceIdType.MESH,
    )
    swap.start()

    chosen = jnp.concatenate([sub[s : s + 1, :] for s in range(ns)], axis=1)
    keep.wait()
    swap.wait()
    sides = []
    for iq in range(2):
        cols = []
        for s in range(ns):
            cols.append(
                jnp.concatenate([jnp.transpose(wfull[h, s, iq]) for h in range(2)], axis=0)
            )
        sides.append(cols)
    for s in range(ns):
        w_r, w_i = sides[0][s], sides[1][s]
        top = jnp.concatenate([w_r, -w_i], axis=1)
        low = jnp.concatenate([w_i, w_r], axis=1)
        wq[s] = jnp.concatenate([top, low], axis=0)
        hi, lo = split(jnp.concatenate([w_r, w_i], axis=0))
        wst[s, 0] = hi
        wst[s, 1] = lo
    flat = jnp.concatenate([jnp.concatenate(cols, axis=1) for cols in sides], axis=0)
    w_hi, w_lo = split(flat)
    for ch in range(2):
        r = lax.broadcasted_iota(jnp.int32, (rows, chans), 0)
        if c_loc % 8 == 0:
            chan = r + ch * rows
        else:
            chan = (ch * half + r % half) * c_loc + r // half
        pick = jnp.where(chan == chosen, 1.0, 0.0).astype(F32)
        pick_b = pick.astype(BF16)
        lhs[ch, 0:chans, :] = jnp.transpose(pick).astype(BF16)
        lhs[ch, chans : chans + 2 * beams, :] = dot_t(w_hi, pick_b).astype(BF16)
        lhs[ch, chans + 2 * beams : chans + 4 * beams, :] = dot_t(w_lo, pick_b).astype(BF16)

    lanes = GB * pulses
    e_re = e_im = None
    for q in range(2):
        mine = me // half
        ch = mine if q == 0 else 1 - mine

        def arrive(t, c):
            src = partner(me, t, n)
            piece(src, src, src).wait_recv()
            return c

        lax.fori_loop(1 if q == 0 else half, half if q == 0 else n, arrive, 0)
        parts = []
        for iq in range(2):
            for g in range(GB):
                j = (g * 2 + iq) * c_loc
                if c_loc % 8 == 0:
                    block = recv[pl.ds(ch * half, half), j : j + c_loc, :].reshape(rows, pulses)
                else:
                    block = jnp.concatenate(
                        [
                            recv[pl.ds(ch * half, half), j + c : j + c + 1, :].reshape(half, pulses)
                            for c in range(c_loc)
                        ],
                        axis=0,
                    )
                parts.append(block)
        z = jnp.concatenate(parts, axis=1)
        z_hi, z_lo = split(z)
        l_hi = lhs[ch, chans : chans + 2 * beams, :]
        l_lo = lhs[ch, chans + 2 * beams : chans + 4 * beams, :]
        part = dot(l_hi, z_hi) + (dot(l_hi, z_lo) + dot(l_lo, z_hi))
        if q == 0:
            sacc[...] = part
        else:
            full = sacc[...] + part
            e_re = full[:beams, :lanes] + full[beams:, lanes:]
            e_im = full[:beams, lanes:] - full[beams:, :lanes]
            p_hi, p_lo = split(e_re * e_re + e_im * e_im)
            ones = jnp.ones((8, lanes), BF16)
            esum = dot_t(ones, p_hi) + dot_t(ones, p_lo)
            esend[...] = esum
            erecv[me] = esum

            def share(t, c):
                d = partner(me, t, n)
                report(d, me, d).start()
                return c

            def report(d, slot, dev):
                return pltpu.make_async_remote_copy(
                    src_ref=esend,
                    dst_ref=erecv.at[slot],
                    send_sem=esend_sem.at[d],
                    recv_sem=erecv_sem.at[slot],
                    device_id=where(dev),
                    device_id_type=pl.DeviceIdType.MESH,
                )

            lax.fori_loop(1, n, share, 0)
        sel = lhs[ch, 0:chans, :]
        g_hi, g_lo = dot(sel, z_hi), dot(sel, z_lo)
        if q == 0:
            gacc[0] = g_hi
            gacc[1] = g_lo
        else:
            gacc[0] = gacc[0] + g_hi
            gacc[1] = gacc[1] + g_lo

    factor = 1.0 / lanes
    lane = lax.broadcasted_iota(jnp.int32, (1, 2 * lanes), 1)
    first = trn[0].astype(F32)
    second = trn[1].astype(F32)
    gate = (lane // pulses) % GB
    mask = jnp.where(gate == 0, first, second)
    power = jnp.zeros((beams, 2 * s_n), F32)
    for s in range(ns):
        x = [gacc[i, s * s_n : (s + 1) * s_n, :] for i in range(2)]
        left = [(v * mask).astype(BF16) for v in x]
        right = [
            jnp.concatenate(
                [v, jnp.concatenate([-v[:, lanes:], v[:, :lanes]], axis=1)], axis=0
            ).astype(BF16)
            for v in x
        ]
        r_s = (
            dot_t(left[0], right[0]) + (dot_t(left[0], right[1]) + dot_t(left[1], right[0]))
        ) * factor
        cov[s] = r_s
        r_hi, r_lo = split(r_s)
        w_h, w_l = wst[s, 0], wst[s, 1]
        t_s = (dot(w_h, r_hi) + (dot(w_h, r_lo) + dot(w_l, r_hi))) * wq[s]
        power = power + t_s[:beams] + t_s[beams:]
    quadratic = jnp.sum(power, axis=1, keepdims=True)
    inverse = 1.0 / jnp.sqrt(quadratic + loading)
    for g in range(GB):
        filt[0, pl.ds(g, beams, stride=GB), :] = e_re[:, g * pulses : (g + 1) * pulses] * inverse
        filt[1, pl.ds(g, beams, stride=GB), :] = e_im[:, g * pulses : (g + 1) * pulses] * inverse

    def close(t, c):
        d = partner(me, t, n)
        report(d, d, d).wait_recv()
        report(d, d, d).wait_send()
        piece(d, d, d).wait_send()
        return c

    lax.fori_loop(1, n, close, 0)
    total = jnp.sum(erecv[...], axis=0)
    en[...] = total[0:1, :] * (1.0 / (gates * pulses))


def body(samples, beam_weights, subarrays, training):
    range_count = lax.axis_size("range")
    cores = lax.axis_size("sub")
    n = range_count * cores
    parts_iq, c_loc, gates, pulses = samples.shape
    blocks, ns, _, s_n, k_half = beam_weights.shape
    assert gates == GB * n and blocks == cores == 2 and subarrays.shape[0] == 1
    assert n & (n - 1) == 0
    assert parts_iq == 2 and n * c_loc == ns * s_n
    beams, chans, lanes = 2 * k_half, n * c_loc, GB * pulses
    dims = (n, cores, c_loc, gates, pulses, ns, s_n, k_half)
    hbm = pl.BlockSpec(memory_space=pl.ANY)
    vmem = pl.BlockSpec(memory_space=pltpu.VMEM)
    dma = pltpu.SemaphoreType.DMA
    cov, filt, en = pl.pallas_call(
        functools.partial(kernel, dims),
        out_shape=(
            jax.ShapeDtypeStruct((ns, s_n, 2 * s_n), F32),
            jax.ShapeDtypeStruct((2, beams * GB, pulses), F32),
            jax.ShapeDtypeStruct((1, beams), F32),
        ),
        in_specs=[hbm, hbm, vmem, pl.BlockSpec(memory_space=pltpu.SMEM)],
        out_specs=(vmem, vmem, vmem),
        scratch_shapes=[
            pltpu.VMEM((2 * c_loc * gates, pulses), F32),
            pltpu.VMEM((n, 2 * GB * c_loc, pulses), F32),
            pltpu.VMEM((n, 2 * GB * c_loc, pulses), F32),
            pltpu.VMEM((2, ns, 2, s_n, k_half), F32),
            pltpu.VMEM((2, chans + 4 * beams, chans // 2), BF16),
            pltpu.VMEM((ns, 2, 2 * beams, s_n), BF16),
            pltpu.VMEM((ns, 2 * beams, 2 * s_n), F32),
            pltpu.VMEM((2 * beams, 2 * lanes), F32),
            pltpu.VMEM((2, chans, 2 * lanes), F32),
            pltpu.VMEM((8, beams), F32),
            pltpu.VMEM((n, 8, beams), F32),
            dma((n,)),
            dma((n,)),
            dma((2,)),
            dma((n,)),
            dma((n,)),
            dma((2,)),
        ],
        compiler_params=pltpu.CompilerParams(collective_id=0, has_side_effects=True),
    )(
        samples.reshape(2 * c_loc * gates, pulses),
        beam_weights,
        subarrays.reshape(ns, s_n),
        training,
    )
    return (
        cov.reshape(1, ns, s_n, 2 * s_n),
        filt.reshape(2, beams, GB, pulses),
        en.reshape(beams),
    )


def solution(mesh):
    placed = (
        P(None, ("groups", "range", "sub"), None, None),
        P(("groups", "range"), None, None, None, "sub"),
        P(("groups", "range", "sub"), None, None),
        P(("groups", "range", "sub")),
    )
    return jax.shard_map(
        body,
        mesh=mesh,
        in_specs=placed,
        out_specs=(
            P(("groups", "range", "sub"), None, None, None),
            P(None, None, ("groups", "range", "sub"), None),
            P("groups"),
        ),
        check_vma=False,
    )
```

```python
import functools

import jax
import jax.numpy as jnp
from jax import lax
from jax.experimental import pallas as pl
from jax.experimental.pallas import tpu as pltpu
from jax.sharding import PartitionSpec as P

GB = 2
loading = 0.05
F32 = jnp.float32
BF16 = jnp.bfloat16


def split(x):
    hi = x.astype(BF16)
    return hi, (x - hi.astype(F32)).astype(BF16)


def dot(a, b):
    return jnp.dot(a, b, preferred_element_type=F32)


def dot_t(a, b):
    return lax.dot_general(a, b, (((1,), (1,)), ((), ())), preferred_element_type=F32)


def partner(me, step, count):
    other, bit = me, 1
    while bit < count:
        other = other + ((step // bit) % 2) * (1 - 2 * ((me // bit) % 2)) * bit
        bit *= 2
    return other


def kernel(
    dims,
    smp, bw, sub_in, trn_in,
    cov, filt, en,
    sub, trn, stage, sendb, recv, wfull, lhs, wst, wq, sacc, gacc, esend, erecv,
    send_sem, recv_sem, wsem, esend_sem, erecv_sem, lsem,
):
    n, cores, c_loc, gates, pulses, ns, s_n, k_half = dims
    beams = 2 * k_half
    chans = n * c_loc
    part = n // 4
    rows = part * c_loc
    core = lax.axis_index("sub")
    me = lax.axis_index("range") * cores + core

    def where(d):
        return {"range": d // cores, "sub": d % cores}

    barrier = pltpu.get_barrier_semaphore()

    def greet(t, c):
        pl.semaphore_signal(
            barrier,
            inc=1,
            device_id=where(partner(me, n - t, n)),
            device_id_type=pl.DeviceIdType.MESH,
        )
        return c

    lax.fori_loop(1, n, greet, 0)
    load = pltpu.make_async_copy(smp, stage, lsem.at[0])
    load.start()
    keep = pltpu.make_async_copy(bw.at[core], wfull.at[core], lsem.at[1])
    keep.start()

    small = [
        pltpu.make_async_copy(sub_in, sub, lsem.at[2]),
        pltpu.make_async_copy(trn_in, trn, lsem.at[3]),
    ]
    for copy in small:
        copy.start()
    load.wait()

    def arrange(d, c):
        for g in range(GB):
            sendb[d, g * 2 * c_loc : (g + 1) * 2 * c_loc, :] = stage[
                pl.ds(d * GB + g, 2 * c_loc, stride=gates), :
            ]
        return c

    lax.fori_loop(0, n, arrange, 0)
    recv[me] = sendb[me]
    pl.semaphore_wait(barrier, n - 1)

    def piece(d, slot, dev):
        return pltpu.make_async_remote_copy(
            src_ref=sendb.at[d],
            dst_ref=recv.at[slot],
            send_sem=send_sem.at[d],
            recv_sem=recv_sem.at[slot],
            device_id=where(dev),
            device_id_type=pl.DeviceIdType.MESH,
        )

    def launch(t, c):
        d = partner(me, t, n)
        piece(d, me, d).start()
        return c

    lax.fori_loop(n // 2, n, launch, 0)
    lax.fori_loop(1, n // 2, launch, 0)
    swap = pltpu.make_async_remote_copy(
        src_ref=bw.at[1 - core],
        dst_ref=wfull.at[core],
        send_sem=wsem.at[0],
        recv_sem=wsem.at[1],
        device_id={"sub": 1 - core},
        device_id_type=pl.DeviceIdType.MESH,
    )
    swap.start()

    for copy in small:
        copy.wait()
    keep.wait()
    swap.wait()
    chosen = jnp.concatenate([sub[s : s + 1, :] for s in range(ns)], axis=1)
    sides = []
    for iq in range(2):
        cols = []
        for s in range(ns):
            cols.append(
                jnp.concatenate([jnp.transpose(wfull[h, s, iq]) for h in range(2)], axis=0)
            )
        sides.append(cols)
    for s in range(ns):
        w_r, w_i = sides[0][s], sides[1][s]
        top = jnp.concatenate([w_r, -w_i], axis=1)
        low = jnp.concatenate([w_i, w_r], axis=1)
        wq[s] = jnp.concatenate([top, low], axis=0)
        hi, lo = split(jnp.concatenate([w_r, w_i], axis=0))
        wst[s, 0] = hi
        wst[s, 1] = lo
    flat = jnp.concatenate([jnp.concatenate(cols, axis=1) for cols in sides], axis=0)
    w_hi, w_lo = split(flat)
    for ch in range(4):
        r = lax.broadcasted_iota(jnp.int32, (rows, chans), 0)
        if c_loc % 8 == 0:
            chan = r + ch * rows
        else:
            chan = (ch * part + r % part) * c_loc + r // part
        pick = jnp.where(chan == chosen, 1.0, 0.0).astype(F32)
        pick_b = pick.astype(BF16)
        lhs[ch, 0:chans, :] = jnp.transpose(pick).astype(BF16)
        lhs[ch, chans : chans + 2 * beams, :] = dot_t(w_hi, pick_b).astype(BF16)
        lhs[ch, chans + 2 * beams : chans + 4 * beams, :] = dot_t(w_lo, pick_b).astype(BF16)

    lanes = GB * pulses
    e_re = e_im = None
    for q in (0, 1, 2, 3):
        ch = partner(me // part, q, 4)

        def arrive(t, c):
            src = partner(me, t, n)
            piece(src, src, src).wait_recv()
            return c

        lax.fori_loop(max(1, q * part), (q + 1) * part, arrive, 0)
        parts = []
        for iq in range(2):
            for g in range(GB):
                j = (g * 2 + iq) * c_loc
                if c_loc % 8 == 0:
                    block = recv[pl.ds(ch * part, part), j : j + c_loc, :].reshape(rows, pulses)
                else:
                    block = jnp.concatenate(
                        [
                            recv[pl.ds(ch * part, part), j + c : j + c + 1, :].reshape(part, pulses)
                            for c in range(c_loc)
                        ],
                        axis=0,
                    )
                parts.append(block)
        z = jnp.concatenate(parts, axis=1)
        z_hi, z_lo = split(z)
        l_hi = lhs[ch, chans : chans + 2 * beams, :]
        l_lo = lhs[ch, chans + 2 * beams : chans + 4 * beams, :]
        term = dot(l_hi, z_hi) + (dot(l_hi, z_lo) + dot(l_lo, z_hi))
        if q == 0:
            sacc[...] = term
        elif q != 3:
            sacc[...] = sacc[...] + term
        else:
            full = sacc[...] + term
            e_re = full[:beams, :lanes] + full[beams:, lanes:]
            e_im = full[:beams, lanes:] - full[beams:, :lanes]
            p_hi, p_lo = split(e_re * e_re + e_im * e_im)
            ones = jnp.ones((8, lanes), BF16)
            esum = (dot_t(ones, p_hi) + dot_t(ones, p_lo))[0:1]
            esend[...] = esum
            erecv[me] = esum

            def share(t, c):
                d = partner(me, n - t, n)
                report(d, me, d).start()
                return c

            def report(d, slot, dev):
                return pltpu.make_async_remote_copy(
                    src_ref=esend,
                    dst_ref=erecv.at[slot],
                    send_sem=esend_sem.at[d],
                    recv_sem=erecv_sem.at[slot],
                    device_id=where(dev),
                    device_id_type=pl.DeviceIdType.MESH,
                )

            lax.fori_loop(1, n, share, 0)
        sel = lhs[ch, 0:chans, :]
        g_hi, g_lo = dot(sel, z_hi), dot(sel, z_lo)
        if q == 0:
            gacc[0] = g_hi
            gacc[1] = g_lo
        else:
            gacc[0] = gacc[0] + g_hi
            gacc[1] = gacc[1] + g_lo

    factor = 1.0 / lanes
    lane = lax.broadcasted_iota(jnp.int32, (1, 2 * lanes), 1)
    first = trn[0].astype(F32)
    second = trn[1].astype(F32)
    gate = (lane // pulses) % GB
    mask = jnp.where(gate == 0, first, second)
    power = jnp.zeros((beams, 2 * s_n), F32)
    for s in range(ns):
        x = [gacc[i, s * s_n : (s + 1) * s_n, :] for i in range(2)]
        left = [(v * mask).astype(BF16) for v in x]
        right = [
            jnp.concatenate(
                [v, jnp.concatenate([-v[:, lanes:], v[:, :lanes]], axis=1)], axis=0
            ).astype(BF16)
            for v in x
        ]
        r_s = (
            dot_t(left[0], right[0]) + (dot_t(left[0], right[1]) + dot_t(left[1], right[0]))
        ) * factor
        cov[s] = r_s
        r_hi, r_lo = split(r_s)
        w_h, w_l = wst[s, 0], wst[s, 1]
        t_s = (dot(w_h, r_hi) + (dot(w_h, r_lo) + dot(w_l, r_hi))) * wq[s]
        power = power + t_s[:beams] + t_s[beams:]
    quadratic = jnp.sum(power, axis=1, keepdims=True)
    inverse = 1.0 / jnp.sqrt(quadratic + loading)
    for g in range(GB):
        filt[0, pl.ds(g, beams, stride=GB), :] = e_re[:, g * pulses : (g + 1) * pulses] * inverse
        filt[1, pl.ds(g, beams, stride=GB), :] = e_im[:, g * pulses : (g + 1) * pulses] * inverse

    def close(t, c):
        d = partner(me, t, n)
        report(d, d, d).wait_recv()
        report(d, d, d).wait_send()
        piece(d, d, d).wait_send()
        return c

    lax.fori_loop(1, n, close, 0)
    total = jnp.sum(erecv[...], axis=0)
    en[...] = total * (1.0 / (gates * pulses))


def store(cov, filt, en, cov_out, filt_out, en_out, sem):
    pairs = ((cov, cov_out), (filt, filt_out), (en, en_out))
    copies = [pltpu.make_async_copy(a, b, sem.at[i]) for i, (a, b) in enumerate(pairs)]
    for copy in copies:
        copy.start()
    for copy in copies:
        copy.wait()


def body(samples, beam_weights, subarrays, training):
    range_count = lax.axis_size("range")
    cores = lax.axis_size("sub")
    n = range_count * cores
    parts_iq, c_loc, gates, pulses = samples.shape
    blocks, ns, _, s_n, k_half = beam_weights.shape
    assert gates == GB * n and blocks == cores == 2 and subarrays.shape[0] == 1
    assert n & (n - 1) == 0
    assert parts_iq == 2 and n * c_loc == ns * s_n
    beams, chans, lanes = 2 * k_half, n * c_loc, GB * pulses
    dims = (n, cores, c_loc, gates, pulses, ns, s_n, k_half)
    hbm = pl.BlockSpec(memory_space=pl.ANY)
    vmem = pl.BlockSpec(memory_space=pltpu.VMEM)
    dma = pltpu.SemaphoreType.DMA
    cov, filt, en = pl.pallas_call(
        functools.partial(kernel, dims),
        out_shape=(
            pltpu.VMEM((ns, s_n, 2 * s_n), F32),
            pltpu.VMEM((2, beams * GB, pulses), F32),
            pltpu.VMEM((1, beams), F32),
        ),
        in_specs=[hbm] * 4,
        out_specs=(vmem, vmem, vmem),
        scratch_shapes=[
            pltpu.VMEM((ns, s_n), jnp.int32),
            pltpu.SMEM((GB,), jnp.int32),
            pltpu.VMEM((2 * c_loc * gates, pulses), F32),
            pltpu.VMEM((n, 2 * GB * c_loc, pulses), F32),
            pltpu.VMEM((n, 2 * GB * c_loc, pulses), F32),
            pltpu.VMEM((2, ns, 2, s_n, k_half), F32),
            pltpu.VMEM((4, chans + 4 * beams, chans // 4), BF16),
            pltpu.VMEM((ns, 2, 2 * beams, s_n), BF16),
            pltpu.VMEM((ns, 2 * beams, 2 * s_n), F32),
            pltpu.VMEM((2 * beams, 2 * lanes), F32),
            pltpu.VMEM((2, chans, 2 * lanes), F32),
            pltpu.VMEM((1, beams), F32),
            pltpu.VMEM((n, 1, beams), F32),
            dma((n,)),
            dma((n,)),
            dma((2,)),
            dma((n,)),
            dma((n,)),
            dma((4,)),
        ],
        compiler_params=pltpu.CompilerParams(collective_id=0, has_side_effects=True),
    )(
        samples.reshape(2 * c_loc * gates, pulses),
        beam_weights,
        subarrays.reshape(ns, s_n),
        training,
    )
    cov, filt, en = (pltpu.with_memory_space_constraint(v, pltpu.VMEM) for v in (cov, filt, en))
    cov, filt, en = pl.pallas_call(
        store,
        out_shape=[jax.ShapeDtypeStruct(v.shape, F32) for v in (cov, filt, en)],
        in_specs=[vmem] * 3,
        out_specs=[hbm] * 3,
        scratch_shapes=[dma((3,))],
    )(cov, filt, en)
    return (
        cov.reshape(1, ns, s_n, 2 * s_n),
        filt.reshape(2, beams, GB, pulses),
        en.reshape(beams),
    )


def solution(mesh):
    placed = (
        P(None, ("groups", "range", "sub"), None, None),
        P(("groups", "range"), None, None, None, "sub"),
        P(("groups", "range", "sub"), None, None),
        P(("groups", "range", "sub")),
    )
    return jax.shard_map(
        body,
        mesh=mesh,
        in_specs=placed,
        out_specs=(
            P(("groups", "range", "sub"), None, None, None),
            P(None, None, ("groups", "range", "sub"), None),
            P("groups"),
        ),
        check_vma=False,
    )
```
